128 devices in a mesh: bond: 32 (over x, z_lo, y), outer: 4 (over z_hi, core).
Axes of the slice: x: 4, y: 4, z: 4 (z_hi: 2, z_lo: 2; z = z_hi * 2 + z_lo), core: 2. Of those that a mesh axis runs over, the one named last changes fastest.
Arguments:
- upper: bfloat16 [128, 128, 128], P(None, 'bond'), may hold values from -4 to 4
- lower: bfloat16 [128, 128, 8, 128], P(None, 'bond', 'outer'), may hold values from -4 to 4
- isometry: bfloat16 [16384, 128], P(('bond', 'outer')), may hold values from -0.046875 to 0.046875
Outputs:
- coarse: float32 [128, 8, 128], P('bond', 'outer')
The draws below stay inside these ranges and needn't reach their ends.
All inputs are finite; a program needn't handle non-finite values.
Results may differ from the reference program's by a relative error of at most 0.004.
Values may be sent and summed in bfloat16 or wider, within the bound.
No kernel may reach another device: no remote copies, remote signals or barrier semaphores. Data moves between devices by JAX's collectives and lax.ppermute only.
A program may use at most 64 MiB of HBM per device.

```python
import jax
import jax.numpy as jnp
from jax import lax

D = 128
LOW = 8


def block_scale(stream_key, extent, split, smallest, high):
    level = 1.0
    for axis_at, blocks in split:
        heights = jax.random.uniform(jax.random.fold_in(jax.random.fold_in(stream_key, 6), axis_at), (blocks,), jnp.float32, smallest / len(split), high / len(split))
        level = level * jnp.repeat(jnp.exp(heights), extent[axis_at] // blocks).reshape((-1,) + (1,) * (len(extent) - 1 - axis_at))
    return level


def bell_draw(stream_key, dims, scale, limit, shards=(), kind=jnp.bfloat16):
    values = scale * jax.random.normal(stream_key, dims, jnp.float32)
    if shards:
        values = values * block_scale(stream_key, dims, shards, -0.22, 0.18)
    return jnp.clip(values, -limit, limit).astype(kind)


def setup_inputs(seed: int = 0) -> dict:
    arg_keys = jax.random.split(jax.random.key(seed), 4)
    upper = bell_draw(arg_keys[0], (D, D, D), 0.3, 4.0, ((1, 32),))
    lower = bell_draw(arg_keys[1], (D, D, LOW, D), 0.3, 4.0, ((1, 32), (2, 4)))
    isometry = bell_draw(arg_keys[2], (D * D, D), (D * D) ** -0.5, 0.046875, ((0, 128),))
    return {"upper": upper, "lower": lower, "isometry": isometry}


def reference(upper, lower, isometry):
    iso_full = isometry.astype(jnp.float32).reshape(D, D, D)

    def member(total, slabs):
        upper_slab, lower_slab = slabs
        joined = jnp.einsum("lr,lkx->rkx", upper_slab.astype(jnp.float32), iso_full).astype(jnp.bfloat16)
        paired = jnp.einsum("rkx,kds->drxs", joined.astype(jnp.float32), lower_slab.astype(jnp.float32)).astype(jnp.bfloat16)
        partial_sum = jnp.einsum("drxs,rsy->xdy", paired.astype(jnp.float32), iso_full)
        return total + partial_sum, None

    start = jnp.zeros((D, LOW, D), jnp.float32)
    result, unused = lax.scan(member, start, (upper, lower))
    return result
```

```python
import jax
import jax.numpy as jnp
from jax import lax
from jax.experimental import pallas as pl
from jax.experimental.pallas import tpu as pltpu
from jax.sharding import Mesh, PartitionSpec as P

SIZES = (4, 2, 4, 2, 2)
NAMES = ("x", "zl", "y", "zh", "c")
BF16 = jnp.bfloat16
F32 = jnp.float32


def from_everyone(value, axes, peers):
    return lax.all_to_all(
        jnp.broadcast_to(value[None], (peers, *value.shape)), axes, 0, 0, tiled=True
    )


def swapped(value, axis):
    return lax.ppermute(value, axis, [(0, 1), (1, 0)])


def along_z(value, shift):
    def at(z):
        return (z % 2) * 2 + z // 2

    return lax.ppermute(
        value, ("zl", "zh"), [(at(z), at((z + shift) % 4)) for z in range(4)]
    )


def mm(a, b):
    return lax.dot_general(a, b, (((1,), (0,)), ((), ())), preferred_element_type=F32)


QB = 4


def step_kernel(z_ref, w_ref, u_ref, wr_ref, l0, l1, l2, l3, acc_ref, out_ref, wt, lower):
    step = pl.program_id(0)

    @pl.when(step == 0)
    def _():
        out_ref[...] = acc_ref[...]
        for k in range(8):
            wt[k * 128 : (k + 1) * 128, :] = w_ref[k].T
        for shift, ref in enumerate((l0, l1, l2, l3)):
            z = (z_ref[0] + 4 - shift) % 4
            for j in range(4):
                row = pl.multiple_of(((z % 2) * 4 + j) * 128, 128)
                for e in range(2):
                    lower[z // 2, pl.ds(row, 128), e * 128 : (e + 1) * 128] = ref[j, e]

    pairs = []
    for half in range(QB // 2):
        u = jnp.concatenate([u_ref[2 * half], u_ref[2 * half + 1]], axis=1)
        joined = mm(wt[...], u).astype(BF16)
        for q in range(2):
            part = joined[:, q * 128 : (q + 1) * 128]
            pairs.append(
                jnp.concatenate([part[k * 128 : (k + 1) * 128] for k in range(8)], axis=1)
            )
    left = jnp.concatenate(pairs, axis=0)
    for zh in range(2):
        paired = mm(left, lower[zh]).astype(BF16)
        for e in range(2):
            rows = jnp.concatenate(
                [
                    paired[q * 128 : (q + 1) * 128, e * 128 : (e + 1) * 128]
                    for q in range(QB)
                ],
                axis=1,
            )
            out_ref[2 * zh + e] += mm(rows, wr_ref[...].reshape(QB * 128, 128))


def contract(z, w, u, wr, lowers, acc):
    whole3 = pl.BlockSpec((8, 128, 128), lambda i: (0, 0, 0))
    block = pl.BlockSpec((QB, 128, 128), lambda i: (i, 0, 0))
    whole_l = pl.BlockSpec((4, 2, 128, 128), lambda i: (0, 0, 0, 0))
    whole_o = pl.BlockSpec((4, 128, 128), lambda i: (0, 0, 0))
    return pl.pallas_call(
        step_kernel,
        grid=(u.shape[0] // QB,),
        in_specs=[pl.BlockSpec(memory_space=pltpu.SMEM), whole3, block, block]
        + [whole_l] * 4
        + [whole_o],
        out_specs=whole_o,
        out_shape=jax.ShapeDtypeStruct((4, 128, 128), F32),
        scratch_shapes=[
            pltpu.VMEM((1024, 128), BF16),
            pltpu.VMEM((2, 1024, 256), BF16),
        ],
        compiler_params=pltpu.CompilerParams(
            dimension_semantics=("arbitrary",), vmem_limit_bytes=40 * 1024 * 1024
        ),
        cost_estimate=pl.CostEstimate(
            flops=4 * 10**9, bytes_accessed=4 * 2**20, transcendentals=0
        ),
        name="contract",
    )(z, w, u, wr, *lowers, acc)


def on_device(upper, lower, isometry):
    zl = lax.axis_index("zl")
    zh = lax.axis_index("zh")
    c = lax.axis_index("c")

    column = from_everyone(isometry, ("zl", "zh", "c"), 8)

    t = jnp.arange(32)
    plane = jnp.where(t < 16, zl, 1 - zl)
    xy = t % 16
    wanted = 4 * ((xy // 4) * 8 + plane * 4 + xy % 4) + 2 * zh + c
    pick = (wanted[:, None] == jnp.arange(128)[None, :]).astype(BF16)
    rights = jnp.einsum(
        "qr,mlr->qlm", pick, upper, preferred_element_type=F32
    ).astype(BF16)
    mine, theirs = rights[:16], swapped(rights[16:], "zl")
    first = jnp.where(zl == 0, mine, theirs)
    second = jnp.where(zl == 0, theirs, mine)
    rights = jnp.concatenate([first, second], axis=1)

    lefts = column.reshape(8, 4, 2, 4, 4, 128)
    lefts = lefts.transpose(1, 3, 2, 4, 0, 5).reshape(16, 64, 128)
    send = jnp.concatenate(
        [
            jnp.broadcast_to(rights.reshape(1, 128, 128), (16, 128, 128)),
            lefts,
            jnp.broadcast_to(isometry[None], (16, 128, 128)),
        ],
        axis=1,
    )
    lower_t = lower.transpose(1, 2, 0, 3)
    lower_t, send = lax.optimization_barrier((lower_t, send))
    got = lax.all_to_all(send, ("x", "y"), 0, 0, tiled=True)
    lowers = [lower_t] + [along_z(lower_t, s) for s in (1, 2, 3)]

    mats = got[:, :192].reshape(16, 24, 8, 128).transpose(1, 0, 2, 3).reshape(24, 128, 128)
    u, w = mats[:16], mats[16:]
    wr = got[:, 192:]
    u_other, wr_other = swapped(u, "c"), swapped(wr, "c")

    z = (2 * zh + zl).astype(jnp.int32)[None]
    acc = contract(z, w, u, wr, lowers, jnp.zeros((4, 128, 128), F32))
    acc = contract(z, w, u_other, wr_other, lowers, acc)

    parts = acc.reshape(2, 2, 32, 4, 128).transpose(2, 0, 3, 1, 4).reshape(64, 4, 2, 128)
    parts = lax.all_to_all(parts, ("x", "zl", "y", "zh"), 0, 0, tiled=True)
    return jnp.sum(parts, axis=0)


def solution(mesh):
    return jax.shard_map(
        on_device,
        mesh=Mesh(mesh.devices.reshape(SIZES), NAMES),
        in_specs=(
            P(None, ("x", "zl", "y"), None),
            P(None, ("x", "zl", "y"), ("zh", "c"), None),
            P(NAMES, None),
        ),
        out_specs=P(("x", "zl", "y"), ("zh", "c"), None),
        check_vma=False,
    )
```

```python
import jax
import jax.numpy as jnp
from jax import lax
from jax.experimental import pallas as pl
from jax.experimental.pallas import tpu as pltpu
from jax.sharding import Mesh, PartitionSpec as P

SIZES = (4, 2, 4, 2, 2)
NAMES = ("x", "zl", "y", "zh", "c")
BF16 = jnp.bfloat16
F32 = jnp.float32


def swapped(value, axis):
    return lax.ppermute(value, axis, [(0, 1), (1, 0)])


def both_swapped(value):
    return lax.ppermute(value, ("zl", "zh"), [(i, 3 - i) for i in range(4)])


def ordered(index, own, other):
    both = jnp.stack([own, other])
    return jnp.where(index == 0, both, both[::-1])


def mm(a, b):
    return lax.dot_general(a, b, (((1,), (0,)), ((), ())), preferred_element_type=F32)


QB = 4


def step_kernel(w_ref, u_ref, wr_ref, l00, l01, l10, l11, acc_ref, out_ref, wt, lower):
    for k in range(8):
        wt[k * 128 : (k + 1) * 128, :] = w_ref[k].T
    for zk, refs in enumerate(((l00, l01), (l10, l11))):
        for zd, ref in enumerate(refs):
            for j in range(4):
                for e in range(2):
                    row, col = (zk * 4 + j) * 128, (zd * 2 + e) * 128
                    lower[row : row + 128, col : col + 128] = ref[j, e]

    for at in range(0, u_ref.shape[0], QB):
        u = jnp.concatenate([u_ref[at + q] for q in range(QB)], axis=1)
        joined = mm(wt[...], u).astype(BF16)
        left = jnp.concatenate(
            [
                jnp.concatenate(
                    [
                        joined[k * 128 : (k + 1) * 128, q * 128 : (q + 1) * 128]
                        for k in range(8)
                    ],
                    axis=1,
                )
                for q in range(QB)
            ],
            axis=0,
        )
        paired = mm(left, lower[...]).astype(BF16)
        rows = jnp.concatenate(
            [
                jnp.concatenate(
                    [
                        paired[q * 128 : (q + 1) * 128, d * 128 : (d + 1) * 128]
                        for q in range(QB)
                    ],
                    axis=1,
                )
                for d in range(4)
            ],
            axis=0,
        )
        part = mm(rows, wr_ref[at : at + QB].reshape(QB * 128, 128)).reshape(4, 128, 128)
        if at == 0:
            out_ref[...] = (part if acc_ref is None else acc_ref[...] + part)
        else:
            out_ref[...] += part


def contract(w, u, wr, lowers, acc):
    vmem = pl.BlockSpec(memory_space=pltpu.VMEM)
    body = step_kernel
    args = [w, u, wr, *lowers]
    if acc is None:

        def body(*refs):
            step_kernel(*refs[:7], None, *refs[7:])
    else:
        args.append(acc)

    return pl.pallas_call(
        body,
        in_specs=[vmem] * len(args),
        out_specs=vmem,
        out_shape=jax.ShapeDtypeStruct((4, 128, 128), F32),
        scratch_shapes=[pltpu.VMEM((1024, 128), BF16), pltpu.VMEM((1024, 512), BF16)],
        compiler_params=pltpu.CompilerParams(vmem_limit_bytes=40 * 1024 * 1024),
        cost_estimate=pl.CostEstimate(
            flops=4 * 10**9, bytes_accessed=4 * 2**20, transcendentals=0
        ),
        name="contract",
    )(*args)


def on_device(upper, lower, isometry):
    zl = lax.axis_index("zl")
    zh = lax.axis_index("zh")
    c = lax.axis_index("c")

    t = jnp.arange(32)
    plane = jnp.where(t < 16, zl, 1 - zl)
    xy = t % 16
    wanted = 4 * ((xy // 4) * 8 + plane * 4 + xy % 4) + 2 * zh + c
    pick = (wanted[:, None] == jnp.arange(128)[None, :]).astype(BF16)
    rights = jnp.einsum(
        "qr,mlr->qlm", pick, upper, preferred_element_type=F32
    ).astype(BF16)
    mine, theirs = rights[:16], swapped(rights[16:], "zl")

    pair = ordered(c, isometry, swapped(isometry, "c"))
    planes = [
        ordered(zh, pair, swapped(pair, "zh")),
        ordered(zh, swapped(pair, "zl"), both_swapped(pair)),
    ]
    column = ordered(zl, *planes).reshape(8, 4, 2, 4, 4, 128)
    ks = column.transpose(1, 3, 2, 4, 0, 5)
    ks = jnp.where(zl == 0, ks, ks[:, :, ::-1])

    l00 = lower.transpose(1, 2, 0, 3)
    l00, ks = lax.optimization_barrier((l00, ks))
    l01 = swapped(l00, "zh")
    l10 = swapped(l00, "zl")
    l11 = both_swapped(l00)
    lowers = (l00, l01, l10, l11)

    first = jnp.where(zl == 0, mine, theirs)
    second = jnp.where(zl == 0, theirs, mine)
    rights = jnp.concatenate([first, second], axis=1)
    send = jnp.concatenate(
        [
            jnp.broadcast_to(rights.reshape(1, 128, 128), (16, 128, 128)),
            ks.reshape(16, 64, 128),
            jnp.broadcast_to(isometry[None], (16, 128, 128)),
        ],
        axis=1,
    )
    got = lax.all_to_all(send, ("x", "y"), 0, 0, tiled=True)
    mats = got[:, :192].reshape(16, 24, 8, 128).transpose(1, 0, 2, 3).reshape(24, 128, 128)
    u, w = mats[:16], mats[16:]
    wr = got[:, 192:]
    u_other, wr_other = swapped(u, "c"), swapped(wr, "c")

    acc = contract(w, u, wr, lowers, None)
    acc = contract(w, u_other, wr_other, lowers, acc)

    parts = acc.reshape(2, 2, 32, 4, 128)
    parts = jnp.where(zh == 0, parts, parts[::-1])
    parts = parts.transpose(2, 0, 3, 1, 4).reshape(64, 4, 2, 128)
    parts = lax.all_to_all(parts, ("x", "zl", "y", "zh"), 0, 0, tiled=True)
    return jnp.sum(parts, axis=0)


def solution(mesh):
    return jax.shard_map(
        on_device,
        mesh=Mesh(mesh.devices.reshape(SIZES), NAMES),
        in_specs=(
            P(None, ("x", "zl", "y"), None),
            P(None, ("x", "zl", "y"), ("zh", "c"), None),
            P(NAMES, None),
        ),
        out_specs=P(("x", "zl", "y"), ("zh", "c"), None),
        check_vma=False,
    )
```

```python
import jax
import jax.numpy as jnp
from jax import lax
from jax.experimental import pallas as pl
from jax.experimental.pallas import tpu as pltpu
from jax.sharding import Mesh, PartitionSpec as P

SIZES = (4, 2, 4, 2, 2)
NAMES = ("x", "zl", "y", "zh", "c")
BF16 = jnp.bfloat16
F32 = jnp.float32


def swapped(value, axis):
    return lax.ppermute(value, axis, [(0, 1), (1, 0)])


def both_swapped(value):
    return lax.ppermute(value, ("zl", "zh"), [(i, 3 - i) for i in range(4)])


def mm(a, b):
    return lax.dot_general(a, b, (((1,), (0,)), ((), ())), preferred_element_type=F32)


QB = 4


def step_kernel(zh_ref, w_ref, u_ref, wr_ref, l00, l01, l10, l11, acc_ref, out_ref, wt, lower):
    for k in range(8):
        wt[k * 128 : (k + 1) * 128, :] = w_ref[k].T
    for zk, refs in enumerate(((l00, l01), (l10, l11))):
        for zd, ref in enumerate(refs):
            for j in range(4):
                for e in range(2):
                    row, col = (zk * 4 + j) * 128, (zd * 2 + e) * 128
                    lower[row : row + 128, col : col + 128] = ref[j, e]

    for at in range(0, u_ref.shape[0], QB):
        u = jnp.concatenate([u_ref[at + q] for q in range(QB)], axis=1)
        joined = mm(wt[...], u).astype(BF16)
        left = jnp.concatenate(
            [
                jnp.concatenate(
                    [
                        joined[k * 128 : (k + 1) * 128, q * 128 : (q + 1) * 128]
                        for k in range(8)
                    ],
                    axis=1,
                )
                for q in range(QB)
            ],
            axis=0,
        )
        paired = mm(left, lower[...]).astype(BF16)
        rows = jnp.concatenate(
            [
                jnp.concatenate(
                    [
                        paired[q * 128 : (q + 1) * 128, d * 128 : (d + 1) * 128]
                        for q in range(QB)
                    ],
                    axis=1,
                )
                for d in range(4)
            ],
            axis=0,
        )
        part = mm(rows, wr_ref[at : at + QB].reshape(QB * 128, 128))
        part = part.reshape(2, 2, 128, 128)
        for zd in range(2):
            to = zh_ref[0] if zd == 0 else 1 - zh_ref[0]
            if at > 0:
                out_ref[to] += part[zd]
            elif acc_ref is None:
                out_ref[to] = part[zd]
            else:
                out_ref[to] = acc_ref[to] + part[zd]


def contract(zh, w, u, wr, lowers, acc):
    vmem = pl.BlockSpec(memory_space=pltpu.VMEM)
    body = step_kernel
    args = [zh, w, u, wr, *lowers]
    if acc is None:

        def body(*refs):
            step_kernel(*refs[:8], None, *refs[8:])
    else:
        args.append(acc)

    return pl.pallas_call(
        body,
        in_specs=[pl.BlockSpec(memory_space=pltpu.SMEM)] + [vmem] * (len(args) - 1),
        out_specs=vmem,
        out_shape=jax.ShapeDtypeStruct((2, 2, 128, 128), F32),
        scratch_shapes=[pltpu.VMEM((1024, 128), BF16), pltpu.VMEM((1024, 512), BF16)],
        compiler_params=pltpu.CompilerParams(vmem_limit_bytes=40 * 1024 * 1024),
        cost_estimate=pl.CostEstimate(
            flops=4 * 10**9, bytes_accessed=4 * 2**20, transcendentals=0
        ),
        name="contract",
    )(*args)


def on_device(upper, lower, isometry):
    zl = lax.axis_index("zl")
    zh = lax.axis_index("zh")
    c = lax.axis_index("c")

    t = jnp.arange(32)
    plane = jnp.where(t < 16, zl, 1 - zl)
    xy = t % 16
    wanted = 4 * ((xy // 4) * 8 + plane * 4 + xy % 4) + 2 * zh + c
    pick = (wanted[:, None] == jnp.arange(128)[None, :]).astype(BF16)
    rights = jnp.einsum(
        "qr,mlr->qlm", pick, upper, preferred_element_type=F32
    ).astype(BF16)
    mine, theirs = rights[:16], swapped(rights[16:], "zl")

    ks = isometry.reshape(4, 2, 4, 4, 128).transpose(0, 2, 1, 3, 4)
    ks = jnp.broadcast_to(ks.reshape(16, 1, 8, 128), (16, 8, 8, 128)).reshape(128, 8, 128)
    w = lax.all_to_all(ks, ("x", "y", "zl", "zh", "c"), 0, 0, tiled=True)

    l00 = lower.transpose(1, 2, 0, 3)
    l01 = swapped(l00, "zh")
    l10 = swapped(l00, "zl")
    l11 = both_swapped(l00)
    lowers = (l00, l01, l10, l11)

    first = jnp.where(zl == 0, mine, theirs)
    second = jnp.where(zl == 0, theirs, mine)
    rights = jnp.concatenate([first, second], axis=1)
    send = jnp.concatenate([rights.reshape(128, 128), isometry], axis=0)
    send, w, *lowers = lax.optimization_barrier((send, w, *lowers))
    send = jnp.broadcast_to(send[None], (16, 256, 128))
    got = lax.all_to_all(send, ("x", "y"), 0, 0, tiled=True)
    w = w.transpose(1, 0, 2).reshape(2, 4, 128, 128)
    w = jnp.where(zl == 0, w, w[::-1]).reshape(8, 128, 128)
    u = got[:, :128].reshape(16, 16, 8, 128).transpose(1, 0, 2, 3).reshape(16, 128, 128)
    wr = got[:, 128:]
    u_other, wr_other = swapped(u, "c"), swapped(wr, "c")

    at = zh.astype(jnp.int32)[None]
    acc = contract(at, w, u, wr, lowers, None)
    acc = contract(at, w, u_other, wr_other, lowers, acc)

    parts = acc.reshape(2, 2, 32, 4, 128).transpose(2, 0, 1, 3, 4).reshape(64, 8, 128)
    parts = lax.all_to_all(parts, ("x", "zl", "y", "zh"), 0, 0, tiled=True)
    return jnp.sum(parts, axis=0).reshape(2, 4, 128).transpose(1, 0, 2)


def solution(mesh):
    return jax.shard_map(
        on_device,
        mesh=Mesh(mesh.devices.reshape(SIZES), NAMES),
        in_specs=(
            P(None, ("x", "zl", "y"), None),
            P(None, ("x", "zl", "y"), ("zh", "c"), None),
            P(NAMES, None),
        ),
        out_specs=P(("x", "zl", "y"), ("zh", "c"), None),
        check_vma=False,
    )
```

```python
import jax
import jax.numpy as jnp
from jax import lax
from jax.experimental import pallas as pl
from jax.experimental.pallas import tpu as pltpu
from jax.sharding import Mesh, PartitionSpec as P

SIZES = (4, 2, 4, 2, 2)
NAMES = ("x", "zl", "y", "zh", "c")
BF16 = jnp.bfloat16
F32 = jnp.float32


def swapped(value, axis):
    return lax.ppermute(value, axis, [(0, 1), (1, 0)])


def both_swapped(value):
    return lax.ppermute(value, ("zl", "zh"), [(i, 3 - i) for i in range(4)])


def ordered(index, own, other):
    both = jnp.stack([own, other])
    return jnp.where(index == 0, both, both[::-1])


def mm(a, b):
    return lax.dot_general(a, b, (((1,), (0,)), ((), ())), preferred_element_type=F32)


QB = 4


def step_kernel(zh_ref, w_ref, u_ref, wr_ref, l00, l01, l10, l11, acc_ref, out_ref, wt, lower):
    for k in range(8):
        wt[k * 128 : (k + 1) * 128, :] = w_ref[k].T
    for zk, refs in enumerate(((l00, l01), (l10, l11))):
        for zd, ref in enumerate(refs):
            for j in range(4):
                for e in range(2):
                    row, col = (zk * 4 + j) * 128, (zd * 2 + e) * 128
                    lower[row : row + 128, col : col + 128] = ref[j, e]

    for at in range(0, u_ref.shape[0], QB):
        u = jnp.concatenate([u_ref[at + q] for q in range(QB)], axis=1)
        joined = mm(wt[...], u).astype(BF16)
        left = jnp.concatenate(
            [
                jnp.concatenate(
                    [
                        joined[k * 128 : (k + 1) * 128, q * 128 : (q + 1) * 128]
                        for k in range(8)
                    ],
                    axis=1,
                )
                for q in range(QB)
            ],
            axis=0,
        )
        paired = mm(left, lower[...]).astype(BF16)
        rows = jnp.concatenate(
            [
                jnp.concatenate(
                    [
                        paired[q * 128 : (q + 1) * 128, d * 128 : (d + 1) * 128]
                        for q in range(QB)
                    ],
                    axis=1,
                )
                for d in range(4)
            ],
            axis=0,
        )
        part = mm(rows, wr_ref[at : at + QB].reshape(QB * 128, 128))
        part = part.reshape(2, 2, 128, 128)
        for zd in range(2):
            to = zh_ref[0] if zd == 0 else 1 - zh_ref[0]
            if at > 0:
                out_ref[to] += part[zd]
            elif acc_ref is None:
                out_ref[to] = part[zd]
            else:
                out_ref[to] = acc_ref[to] + part[zd]


def contract(zh, w, u, wr, lowers, acc):
    vmem = pl.BlockSpec(memory_space=pltpu.VMEM)
    body = step_kernel
    args = [zh, w, u, wr, *lowers]
    if acc is None:

        def body(*refs):
            step_kernel(*refs[:8], None, *refs[8:])
    else:
        args.append(acc)

    return pl.pallas_call(
        body,
        in_specs=[pl.BlockSpec(memory_space=pltpu.SMEM)] + [vmem] * (len(args) - 1),
        out_specs=vmem,
        out_shape=jax.ShapeDtypeStruct((2, 2, 128, 128), F32),
        scratch_shapes=[pltpu.VMEM((1024, 128), BF16), pltpu.VMEM((1024, 512), BF16)],
        compiler_params=pltpu.CompilerParams(vmem_limit_bytes=40 * 1024 * 1024),
        cost_estimate=pl.CostEstimate(
            flops=4 * 10**9, bytes_accessed=4 * 2**20, transcendentals=0
        ),
        name="contract",
    )(*args)


def on_device(upper, lower, isometry):
    zl = lax.axis_index("zl")
    zh = lax.axis_index("zh")
    c = lax.axis_index("c")

    t = jnp.arange(32)
    plane = jnp.where(t < 16, zl, 1 - zl)
    xy = t % 16
    wanted = 4 * ((xy // 4) * 8 + plane * 4 + xy % 4) + 2 * zh + c
    pick = (wanted[:, None] == jnp.arange(128)[None, :]).astype(BF16)
    rights = jnp.einsum(
        "qr,mlr->qlm", pick, upper, preferred_element_type=F32
    ).astype(BF16)
    mine, theirs = rights[:16], swapped(rights[16:], "zl")

    pair = ordered(c, isometry, swapped(isometry, "c"))
    others = [swapped(pair, "zh"), swapped(pair, "zl"), both_swapped(pair)]
    planes = [ordered(zh, pair, others[0]), ordered(zh, *others[1:])]
    column = ordered(zl, *planes).reshape(8, 4, 2, 4, 4, 128)
    ks = column.transpose(1, 3, 2, 4, 0, 5)
    ks = jnp.where(zl == 0, ks, ks[:, :, ::-1])

    l00 = lower.transpose(1, 2, 0, 3)
    l01 = swapped(l00, "zh")
    l10 = swapped(l00, "zl")
    l11 = both_swapped(l00)
    lowers = (l00, l01, l10, l11)

    first = jnp.where(zl == 0, mine, theirs)
    second = jnp.where(zl == 0, theirs, mine)
    rights = jnp.concatenate([first, second], axis=1)
    send = jnp.concatenate(
        [
            jnp.broadcast_to(rights.reshape(1, 128, 128), (16, 128, 128)),
            ks.reshape(16, 64, 128),
            jnp.broadcast_to(isometry[None], (16, 128, 128)),
        ],
        axis=1,
    )
    got = lax.all_to_all(send, ("x", "y"), 0, 0, tiled=True)
    mats = got[:, :192].reshape(16, 24, 8, 128).transpose(1, 0, 2, 3).reshape(24, 128, 128)
    u, w = mats[:16], mats[16:]
    wr = got[:, 192:]
    u_other, wr_other = swapped(u, "c"), swapped(wr, "c")

    at = zh.astype(jnp.int32)[None]
    acc = contract(at, w, u, wr, lowers, None)
    acc = contract(at, w, u_other, wr_other, lowers, acc)

    parts = acc.reshape(2, 2, 32, 4, 128).transpose(2, 0, 1, 3, 4).reshape(64, 8, 128)
    parts = lax.all_to_all(parts, ("x", "zl", "y", "zh"), 0, 0, tiled=True)
    return jnp.sum(parts, axis=0).reshape(2, 4, 128).transpose(1, 0, 2)


def solution(mesh):
    return jax.shard_map(
        on_device,
        mesh=Mesh(mesh.devices.reshape(SIZES), NAMES),
        in_specs=(
            P(None, ("x", "zl", "y"), None),
            P(None, ("x", "zl", "y"), ("zh", "c"), None),
            P(NAMES, None),
        ),
        out_specs=P(("x", "zl", "y"), ("zh", "c"), None),
        check_vma=False,
    )
```

```python
import jax
import jax.numpy as jnp
from jax import lax
from jax.experimental import pallas as pl
from jax.experimental.pallas import tpu as pltpu
from jax.sharding import Mesh, PartitionSpec as P

SIZES = (4, 2, 4, 2, 2)
NAMES = ("x", "zl", "y", "zh", "c")
BF16 = jnp.bfloat16
F32 = jnp.float32


def swapped(value, axis):
    return lax.ppermute(value, axis, [(0, 1), (1, 0)])


def both_swapped(value):
    return lax.ppermute(value, ("zl", "zh"), [(i, 3 - i) for i in range(4)])


def ordered(index, own, other):
    both = jnp.stack([own, other])
    return jnp.where(index == 0, both, both[::-1])


def mm(a, b):
    return lax.dot_general(a, b, (((1,), (0,)), ((), ())), preferred_element_type=F32)


QB = 4


def step_kernel(zh_ref, w_ref, u_ref, wr_ref, near, far, acc_ref, out_ref, wt, lower):
    for k in range(8):
        wt[k * 128 : (k + 1) * 128, :] = w_ref[k].T
    for zk in range(2):
        for j in range(4):
            for e in range(2):
                rows = slice((zk * 4 + j) * 128, (zk * 4 + j + 1) * 128)
                lower[rows, e * 128 : (e + 1) * 128] = near[zk, j, e]
                lower[rows, (e + 2) * 128 : (e + 3) * 128] = far[1 - zk, j, e]

    for at in range(0, u_ref.shape[0], QB):
        u = jnp.concatenate([u_ref[at + q] for q in range(QB)], axis=1)
        joined = mm(wt[...], u).astype(BF16)
        left = jnp.concatenate(
            [
                jnp.concatenate(
                    [
                        joined[k * 128 : (k + 1) * 128, q * 128 : (q + 1) * 128]
                        for k in range(8)
                    ],
                    axis=1,
                )
                for q in range(QB)
            ],
            axis=0,
        )
        paired = mm(left, lower[...]).astype(BF16)
        rows = jnp.concatenate(
            [
                jnp.concatenate(
                    [
                        paired[q * 128 : (q + 1) * 128, d * 128 : (d + 1) * 128]
                        for q in range(QB)
                    ],
                    axis=1,
                )
                for d in range(4)
            ],
            axis=0,
        )
        part = mm(rows, wr_ref[at : at + QB].reshape(QB * 128, 128))
        part = part.reshape(2, 2, 128, 128)
        for zd in range(2):
            to = zh_ref[0] if zd == 0 else 1 - zh_ref[0]
            if at > 0:
                out_ref[to] += part[zd]
            elif acc_ref is None:
                out_ref[to] = part[zd]
            else:
                out_ref[to] = acc_ref[to] + part[zd]


def contract(zh, w, u, wr, lowers, acc):
    vmem = pl.BlockSpec(memory_space=pltpu.VMEM)
    body = step_kernel
    args = [zh, w, u, wr, *lowers]
    if acc is None:

        def body(*refs):
            step_kernel(*refs[:6], None, *refs[6:])
    else:
        args.append(acc)

    return pl.pallas_call(
        body,
        in_specs=[pl.BlockSpec(memory_space=pltpu.SMEM)] + [vmem] * (len(args) - 1),
        out_specs=vmem,
        out_shape=jax.ShapeDtypeStruct((2, 2, 128, 128), F32),
        scratch_shapes=[pltpu.VMEM((1024, 128), BF16), pltpu.VMEM((1024, 512), BF16)],
        compiler_params=pltpu.CompilerParams(vmem_limit_bytes=40 * 1024 * 1024),
        cost_estimate=pl.CostEstimate(
            flops=4 * 10**9, bytes_accessed=4 * 2**20, transcendentals=0
        ),
        name="contract",
    )(*args)


def on_device(upper, lower, isometry):
    zl = lax.axis_index("zl")
    zh = lax.axis_index("zh")
    c = lax.axis_index("c")

    t = jnp.arange(32)
    plane = jnp.where(t < 16, zl, 1 - zl)
    xy = t % 16
    wanted = 4 * ((xy // 4) * 8 + plane * 4 + xy % 4) + 2 * zh + c
    pick = (wanted[:, None] == jnp.arange(128)[None, :]).astype(BF16)
    rights = jnp.einsum(
        "qr,mlr->qlm", pick, upper, preferred_element_type=F32
    ).astype(BF16)
    pair = ordered(c, isometry, swapped(isometry, "c"))
    theirs = swapped(
        jnp.concatenate([rights[16:].reshape(64, 128), pair.reshape(256, 128)]), "zl"
    )
    first, second = ordered(zl, rights[:16], theirs[:64].reshape(16, 4, 128))
    rights = jnp.concatenate([first, second], axis=1)
    near = ordered(zl, pair, theirs[64:].reshape(2, 128, 128))
    far = both_swapped(near)
    column = jnp.stack([ordered(zh, near[i], far[i]) for i in range(2)])
    column = column.reshape(8, 4, 2, 4, 4, 128)
    ks = column.transpose(1, 3, 2, 4, 0, 5)
    ks = jnp.where(zl == 0, ks, ks[:, :, ::-1])

    lower = lower.transpose(1, 2, 0, 3)
    l_near = jnp.stack([lower, swapped(lower, "zl")])
    l_far = both_swapped(l_near)
    lowers = (l_near, l_far)

    send = jnp.concatenate(
        [
            jnp.broadcast_to(rights.reshape(1, 128, 128), (16, 128, 128)),
            ks.reshape(16, 64, 128),
            jnp.broadcast_to(isometry[None], (16, 128, 128)),
        ],
        axis=1,
    )
    got = lax.all_to_all(send, ("x", "y"), 0, 0, tiled=True)
    mats = got[:, :192].reshape(16, 24, 8, 128).transpose(1, 0, 2, 3).reshape(24, 128, 128)
    u, w = mats[:16], mats[16:]
    wr = got[:, 192:]
    u_other, wr_other = swapped(u, "c"), swapped(wr, "c")

    at = zh.astype(jnp.int32)[None]
    acc = contract(at, w, u, wr, lowers, None)
    acc = contract(at, w, u_other, wr_other, lowers, acc)

    parts = acc.reshape(2, 2, 32, 4, 128).transpose(2, 0, 1, 3, 4).reshape(64, 8, 128)
    parts = lax.all_to_all(parts, ("x", "zl", "y", "zh"), 0, 0, tiled=True)
    return jnp.sum(parts, axis=0).reshape(2, 4, 128).transpose(1, 0, 2)


def solution(mesh):
    return jax.shard_map(
        on_device,
        mesh=Mesh(mesh.devices.reshape(SIZES), NAMES),
        in_specs=(
            P(None, ("x", "zl", "y"), None),
            P(None, ("x", "zl", "y"), ("zh", "c"), None),
            P(NAMES, None),
        ),
        out_specs=P(("x", "zl", "y"), ("zh", "c"), None),
        check_vma=False,
    )
```

```python
import jax
import jax.numpy as jnp
from jax import lax
from jax.experimental import pallas as pl
from jax.experimental.pallas import tpu as pltpu
from jax.sharding import Mesh, PartitionSpec as P

SIZES = (4, 2, 4, 2, 2)
NAMES = ("x", "zl", "y", "zh", "c")
BF16 = jnp.bfloat16
F32 = jnp.float32


def from_everyone(value, axes, peers):
    return lax.all_to_all(
        jnp.broadcast_to(value[None], (peers, *value.shape)), axes, 0, 0, tiled=True
    )


def swapped(value, axis):
    return lax.ppermute(value, axis, [(0, 1), (1, 0)])


def both_swapped(value):
    return lax.ppermute(value, ("zl", "zh"), [(i, 3 - i) for i in range(4)])


def mm(a, b):
    return lax.dot_general(a, b, (((1,), (0,)), ((), ())), preferred_element_type=F32)


QB = 4


def step_kernel(zl_ref, zh_ref, w_ref, u0, u1, wr0, wr1, l00, l01, l10, l11, out_ref, wt, lower):
    for k in range(8):
        wt[k * 128 : (k + 1) * 128, :] = w_ref[k].T
    for zk, refs in enumerate(((l00, l01), (l10, l11))):
        plane = zl_ref[0] if zk == 0 else 1 - zl_ref[0]
        for j in range(4):
            row = pl.multiple_of((plane * 4 + j) * 128, 128)
            for zd, ref in enumerate(refs):
                for e in range(2):
                    col = (zd * 2 + e) * 128
                    lower[pl.ds(row, 128), col : col + 128] = ref[j, e]

    for half, (u_ref, wr_ref) in enumerate(((u0, wr0), (u1, wr1))):
        for at in range(0, u_ref.shape[0], QB):
            u = jnp.concatenate([u_ref[at + q] for q in range(QB)], axis=1)
            joined = mm(wt[...], u).astype(BF16)
            left = jnp.concatenate(
                [
                    jnp.concatenate(
                        [
                            joined[k * 128 : (k + 1) * 128, q * 128 : (q + 1) * 128]
                            for k in range(8)
                        ],
                        axis=1,
                    )
                    for q in range(QB)
                ],
                axis=0,
            )
            paired = mm(left, lower[...]).astype(BF16)
            rows = jnp.concatenate(
                [
                    jnp.concatenate(
                        [
                            paired[q * 128 : (q + 1) * 128, d * 128 : (d + 1) * 128]
                            for q in range(QB)
                        ],
                        axis=1,
                    )
                    for d in range(4)
                ],
                axis=0,
            )
            part = mm(rows, wr_ref[at : at + QB].reshape(QB * 128, 128))
            part = part.reshape(2, 2, 128, 128)
            for zd in range(2):
                to = zh_ref[0] if zd == 0 else 1 - zh_ref[0]
                if half + at == 0:
                    out_ref[to] = part[zd]
                else:
                    out_ref[to] += part[zd]


def contract(zl, zh, w, u, wr, lowers):
    vmem = pl.BlockSpec(memory_space=pltpu.VMEM)
    args = [zl, zh, w, *u, *wr, *lowers]
    return pl.pallas_call(
        step_kernel,
        in_specs=[pl.BlockSpec(memory_space=pltpu.SMEM)] * 2 + [vmem] * (len(args) - 2),
        out_specs=vmem,
        out_shape=jax.ShapeDtypeStruct((2, 2, 128, 128), F32),
        scratch_shapes=[pltpu.VMEM((1024, 128), BF16), pltpu.VMEM((1024, 512), BF16)],
        compiler_params=pltpu.CompilerParams(vmem_limit_bytes=40 * 1024 * 1024),
        cost_estimate=pl.CostEstimate(
            flops=8 * 10**9, bytes_accessed=6 * 2**20, transcendentals=0
        ),
        name="contract",
    )(*args)


def on_device(upper, lower, isometry):
    zl = lax.axis_index("zl")
    zh = lax.axis_index("zh")
    c = lax.axis_index("c")

    t = jnp.arange(32)
    plane = jnp.where(t < 16, zl, 1 - zl)
    xy = t % 16
    wanted = 4 * ((xy // 4) * 8 + plane * 4 + xy % 4) + 2 * zh + c
    pick = (wanted[:, None] == jnp.arange(128)[None, :]).astype(BF16)
    rights = jnp.einsum(
        "qr,mlr->qlm", pick, upper, preferred_element_type=F32
    ).astype(BF16)
    theirs = swapped(rights[16:], "zl")
    mine = rights[:16]

    l00 = lower.transpose(1, 2, 0, 3)
    l01 = swapped(l00, "zh")
    l10 = swapped(l00, "zl")
    l11 = both_swapped(l00)
    lowers = (l00, l01, l10, l11)

    first = jnp.where(zl == 0, mine, theirs)
    second = jnp.where(zl == 0, theirs, mine)
    rights = jnp.concatenate([first, second], axis=1)
    ks = isometry.reshape(4, 2, 4, 4, 128).transpose(0, 2, 1, 3, 4)
    send = jnp.concatenate(
        [
            jnp.broadcast_to(rights.reshape(1, 128, 128), (16, 128, 128)),
            jnp.broadcast_to(isometry[None], (16, 128, 128)),
            ks.reshape(16, 8, 128),
        ],
        axis=1,
    )
    got = lax.all_to_all(send, ("x", "y"), 0, 0, tiled=True)
    u = got[:, :128].reshape(16, 16, 8, 128).transpose(1, 0, 2, 3).reshape(16, 128, 128)
    wr = got[:, 128:256]
    u_other, wr_other = swapped(u, "c"), swapped(wr, "c")

    w = from_everyone(got[:, 256:], ("zl", "zh", "c"), 8)
    w = w.transpose(2, 1, 0, 3).reshape(8, 128, 128)

    here = (zl.astype(jnp.int32)[None], zh.astype(jnp.int32)[None])
    acc = contract(*here, w, (u, u_other), (wr, wr_other), lowers)

    parts = acc.reshape(2, 2, 32, 4, 128).transpose(2, 0, 1, 3, 4).reshape(64, 8, 128)
    parts = lax.all_to_all(parts, ("x", "zl", "y", "zh"), 0, 0, tiled=True)
    return jnp.sum(parts, axis=0).reshape(2, 4, 128).transpose(1, 0, 2)


def solution(mesh):
    return jax.shard_map(
        on_device,
        mesh=Mesh(mesh.devices.reshape(SIZES), NAMES),
        in_specs=(
            P(None, ("x", "zl", "y"), None),
            P(None, ("x", "zl", "y"), ("zh", "c"), None),
            P(NAMES, None),
        ),
        out_specs=P(("x", "zl", "y"), ("zh", "c"), None),
        check_vma=False,
    )
```

```python
import jax
import jax.numpy as jnp
from jax import lax
from jax.experimental import pallas as pl
from jax.experimental.pallas import tpu as pltpu
from jax.sharding import Mesh, PartitionSpec as P

SIZES = (4, 2, 4, 2, 2)
NAMES = ("x", "zl", "y", "zh", "c")
BF16 = jnp.bfloat16
F32 = jnp.float32


def from_everyone(value, axes, peers):
    return lax.all_to_all(
        jnp.broadcast_to(value[None], (peers, *value.shape)), axes, 0, 0, tiled=True
    )


def swapped(value, axis):
    return lax.ppermute(value, axis, [(0, 1), (1, 0)])


def both_swapped(value):
    return lax.ppermute(value, ("zl", "zh"), [(i, 3 - i) for i in range(4)])


def ordered(index, own, other):
    both = jnp.stack([own, other])
    return jnp.where(index == 0, both, both[::-1])


def mm(a, b):
    return lax.dot_general(a, b, (((1,), (0,)), ((), ())), preferred_element_type=F32)


QB = 4


def step_kernel(zl_ref, zh_ref, w_ref, u0, u1, wr0, wr1, l00, l01, l10, l11, out_ref, wt, lower):
    for k in range(8):
        wt[k * 128 : (k + 1) * 128, :] = w_ref[k].T
    for zk, refs in enumerate(((l00, l01), (l10, l11))):
        plane = zl_ref[0] if zk == 0 else 1 - zl_ref[0]
        for j in range(4):
            row = pl.multiple_of((plane * 4 + j) * 128, 128)
            for zd, ref in enumerate(refs):
                for e in range(2):
                    col = (zd * 2 + e) * 128
                    lower[pl.ds(row, 128), col : col + 128] = ref[j, e]

    for half, (u_ref, wr_ref) in enumerate(((u0, wr0), (u1, wr1))):
        for at in range(0, u_ref.shape[0], QB):
            u = jnp.concatenate([u_ref[at + q] for q in range(QB)], axis=1)
            joined = mm(wt[...], u).astype(BF16)
            left = jnp.concatenate(
                [
                    jnp.concatenate(
                        [
                            joined[k * 128 : (k + 1) * 128, q * 128 : (q + 1) * 128]
                            for k in range(8)
                        ],
                        axis=1,
                    )
                    for q in range(QB)
                ],
                axis=0,
            )
            paired = mm(left, lower[...]).astype(BF16)
            rows = jnp.concatenate(
                [
                    jnp.concatenate(
                        [
                            paired[q * 128 : (q + 1) * 128, d * 128 : (d + 1) * 128]
                            for q in range(QB)
                        ],
                        axis=1,
                    )
                    for d in range(4)
                ],
                axis=0,
            )
            part = mm(rows, wr_ref[at : at + QB].reshape(QB * 128, 128))
            part = part.reshape(2, 2, 128, 128)
            for zd in range(2):
                to = zh_ref[0] if zd == 0 else 1 - zh_ref[0]
                if half + at == 0:
                    out_ref[to] = part[zd]
                else:
                    out_ref[to] += part[zd]


def contract(zl, zh, w, u, wr, lowers):
    vmem = pl.BlockSpec(memory_space=pltpu.VMEM)
    args = [zl, zh, w, *u, *wr, *lowers]
    return pl.pallas_call(
        step_kernel,
        in_specs=[pl.BlockSpec(memory_space=pltpu.SMEM)] * 2 + [vmem] * (len(args) - 2),
        out_specs=vmem,
        out_shape=jax.ShapeDtypeStruct((2, 2, 128, 128), F32),
        scratch_shapes=[pltpu.VMEM((1024, 128), BF16), pltpu.VMEM((1024, 512), BF16)],
        compiler_params=pltpu.CompilerParams(vmem_limit_bytes=40 * 1024 * 1024),
        cost_estimate=pl.CostEstimate(
            flops=8 * 10**9, bytes_accessed=6 * 2**20, transcendentals=0
        ),
        name="contract",
    )(*args)


def on_device(upper, lower, isometry):
    zl = lax.axis_index("zl")
    zh = lax.axis_index("zh")
    c = lax.axis_index("c")

    t = jnp.arange(32)
    plane = jnp.where(t < 16, zl, 1 - zl)
    xy = t % 16
    wanted = 4 * ((xy // 4) * 8 + plane * 4 + xy % 4) + 2 * zh + c
    pick = (wanted[:, None] == jnp.arange(128)[None, :]).astype(BF16)
    rights = jnp.einsum(
        "qr,mlr->qlm", pick, upper, preferred_element_type=F32
    ).astype(BF16)
    theirs = swapped(
        jnp.concatenate([rights[16:].reshape(64, 128), isometry], axis=0), "zl"
    )
    rights = ordered(zl, rights[:16], theirs[:64].reshape(16, 4, 128))
    rights = rights.transpose(1, 2, 0, 3)
    slabs = ordered(zl, isometry, theirs[64:]).reshape(2, 4, 2, 4, 4, 128)
    ks = slabs.transpose(1, 3, 0, 2, 4, 5)

    l00 = lower.transpose(1, 2, 0, 3)
    l01 = swapped(l00, "zh")
    l10 = swapped(l00, "zl")
    l11 = both_swapped(l00)
    lowers = (l00, l01, l10, l11)

    send = jnp.concatenate(
        [
            jnp.broadcast_to(rights.reshape(1, 128, 128), (16, 128, 128)),
            jnp.broadcast_to(isometry[None], (16, 128, 128)),
            ks.reshape(16, 16, 128),
        ],
        axis=1,
    )
    got = lax.all_to_all(send, ("x", "y"), 0, 0, tiled=True)
    got, *lowers = lax.optimization_barrier((got, *lowers))
    u = got[:, :128].reshape(16, 16, 8, 128).transpose(1, 0, 2, 3).reshape(16, 128, 128)
    wr = got[:, 128:256]
    u_other, wr_other = swapped(u, "c"), swapped(wr, "c")

    mine = got[:, 256:].reshape(16, 2, 8, 128).transpose(1, 2, 0, 3)
    w = from_everyone(mine, ("zh", "c"), 4).reshape(8, 8, 16, 128)
    w = w.transpose(1, 2, 0, 3).reshape(8, 128, 128)

    here = (zl.astype(jnp.int32)[None], zh.astype(jnp.int32)[None])
    acc = contract(*here, w, (u, u_other), (wr, wr_other), lowers)

    parts = acc.reshape(2, 2, 32, 4, 128).transpose(2, 0, 1, 3, 4).reshape(64, 8, 128)
    parts = lax.all_to_all(parts, ("x", "zl", "y", "zh"), 0, 0, tiled=True)
    return jnp.sum(parts, axis=0).reshape(2, 4, 128).transpose(1, 0, 2)


def solution(mesh):
    return jax.shard_map(
        on_device,
        mesh=Mesh(mesh.devices.reshape(SIZES), NAMES),
        in_specs=(
            P(None, ("x", "zl", "y"), None),
            P(None, ("x", "zl", "y"), ("zh", "c"), None),
            P(NAMES, None),
        ),
        out_specs=P(("x", "zl", "y"), ("zh", "c"), None),
        check_vma=False,
    )
```

```python
import jax
import jax.numpy as jnp
from jax import lax
from jax.experimental import pallas as pl
from jax.experimental.pallas import tpu as pltpu
from jax.sharding import Mesh, PartitionSpec as P

SIZES = (4, 2, 4, 2, 2)
NAMES = ("x", "zl", "y", "zh", "c")
BF16 = jnp.bfloat16
F32 = jnp.float32


def swapped(value, axis):
    return lax.ppermute(value, axis, [(0, 1), (1, 0)])


def both_swapped(value):
    return lax.ppermute(value, ("zl", "zh"), [(i, 3 - i) for i in range(4)])


def ordered(index, own, other):
    both = jnp.stack([own, other])
    return jnp.where(index == 0, both, both[::-1])


def mm(a, b):
    return lax.dot_general(a, b, (((1,), (0,)), ((), ())), preferred_element_type=F32)


QB = 4


def step_kernel(zh_ref, w_ref, u_ref, wr_ref, l00, l01, l10, l11, acc_ref, out_ref, wt, lower):
    for k in range(8):
        wt[k * 128 : (k + 1) * 128, :] = w_ref[k].T
    for zk, refs in enumerate(((l00, l01), (l10, l11))):
        for zd, ref in enumerate(refs):
            for j in range(4):
                for e in range(2):
                    row, col = (zk * 4 + j) * 128, (zd * 2 + e) * 128
                    lower[row : row + 128, col : col + 128] = ref[j, e]

    for at in range(0, u_ref.shape[0], QB):
        u = jnp.concatenate([u_ref[at + q] for q in range(QB)], axis=1)
        joined = mm(wt[...], u).astype(BF16)
        left = jnp.concatenate(
            [
                jnp.concatenate(
                    [
                        joined[k * 128 : (k + 1) * 128, q * 128 : (q + 1) * 128]
                        for k in range(8)
                    ],
                    axis=1,
                )
                for q in range(QB)
            ],
            axis=0,
        )
        paired = mm(left, lower[...]).astype(BF16)
        rows = jnp.concatenate(
            [
                jnp.concatenate(
                    [
                        paired[q * 128 : (q + 1) * 128, d * 128 : (d + 1) * 128]
                        for q in range(QB)
                    ],
                    axis=1,
                )
                for d in range(4)
            ],
            axis=0,
        )
        part = mm(rows, wr_ref[at : at + QB].reshape(QB * 128, 128))
        part = part.reshape(2, 2, 128, 128)
        for zd in range(2):
            to = zh_ref[0] if zd == 0 else 1 - zh_ref[0]
            if at > 0:
                out_ref[to] += part[zd]
            elif acc_ref is None:
                out_ref[to] = part[zd]
            else:
                out_ref[to] = acc_ref[to] + part[zd]


def contract(zh, w, u, wr, lowers, acc):
    vmem = pl.BlockSpec(memory_space=pltpu.VMEM)
    body = step_kernel
    args = [zh, w, u, wr, *lowers]
    if acc is None:

        def body(*refs):
            step_kernel(*refs[:8], None, *refs[8:])
    else:
        args.append(acc)

    return pl.pallas_call(
        body,
        in_specs=[pl.BlockSpec(memory_space=pltpu.SMEM)] + [vmem] * (len(args) - 1),
        out_specs=vmem,
        out_shape=jax.ShapeDtypeStruct((2, 2, 128, 128), F32),
        scratch_shapes=[pltpu.VMEM((1024, 128), BF16), pltpu.VMEM((1024, 512), BF16)],
        compiler_params=pltpu.CompilerParams(vmem_limit_bytes=40 * 1024 * 1024),
        cost_estimate=pl.CostEstimate(
            flops=4 * 10**9, bytes_accessed=4 * 2**20, transcendentals=0
        ),
        name="contract",
    )(*args)


def on_device(upper, lower, isometry):
    zl = lax.axis_index("zl")
    zh = lax.axis_index("zh")
    c = lax.axis_index("c")

    lower = lower.transpose(1, 2, 0, 3)
    pair = ordered(c, isometry, swapped(isometry, "c"))
    upper, lower = lax.optimization_barrier((upper, lower))

    t = jnp.arange(32)
    plane = jnp.where(t < 16, zl, 1 - zl)
    xy = t % 16
    wanted = 4 * ((xy // 4) * 8 + plane * 4 + xy % 4) + 2 * zh + c
    pick = (wanted[:, None] == jnp.arange(128)[None, :]).astype(BF16)
    rights = jnp.einsum(
        "qr,mlr->qlm", pick, upper, preferred_element_type=F32
    ).astype(BF16)

    theirs = swapped(
        jnp.concatenate([rights[16:].reshape(64, 128), pair.reshape(256, 128)]), "zl"
    )
    far = swapped(pair, "zh"), both_swapped(pair)
    own = ordered(zh, pair, far[0])
    other = ordered(zh, theirs[64:].reshape(2, 128, 128), far[1])
    column = ordered(zl, own, other).reshape(8, 4, 2, 4, 4, 128)
    ks = column.transpose(1, 3, 2, 4, 0, 5)
    ks = jnp.where(zl == 0, ks, ks[:, :, ::-1])

    lowers = (lower, swapped(lower, "zh"), swapped(lower, "zl"), both_swapped(lower))

    theirs = theirs[:64].reshape(16, 4, 128)
    first = jnp.where(zl == 0, rights[:16], theirs)
    second = jnp.where(zl == 0, theirs, rights[:16])
    rights = jnp.concatenate([first, second], axis=1)
    send = jnp.concatenate(
        [
            jnp.broadcast_to(rights.reshape(1, 128, 128), (16, 128, 128)),
            ks.reshape(16, 64, 128),
            jnp.broadcast_to(isometry[None], (16, 128, 128)),
        ],
        axis=1,
    )
    got = lax.all_to_all(send, ("x", "y"), 0, 0, tiled=True)
    mats = got[:, :192].reshape(16, 24, 8, 128).transpose(1, 0, 2, 3).reshape(24, 128, 128)
    u, w = mats[:16], mats[16:]
    wr = got[:, 192:]
    u_other, wr_other = swapped(u, "c"), swapped(wr, "c")

    at = zh.astype(jnp.int32)[None]
    acc = contract(at, w, u, wr, lowers, None)
    acc = contract(at, w, u_other, wr_other, lowers, acc)

    parts = acc.reshape(2, 2, 32, 4, 128).transpose(2, 0, 1, 3, 4).reshape(64, 8, 128)
    parts = lax.all_to_all(parts, ("x", "zl", "y", "zh"), 0, 0, tiled=True)
    return jnp.sum(parts, axis=0).reshape(2, 4, 128).transpose(1, 0, 2)


def solution(mesh):
    return jax.shard_map(
        on_device,
        mesh=Mesh(mesh.devices.reshape(SIZES), NAMES),
        in_specs=(
            P(None, ("x", "zl", "y"), None),
            P(None, ("x", "zl", "y"), ("zh", "c"), None),
            P(NAMES, None),
        ),
        out_specs=P(("x", "zl", "y"), ("zh", "c"), None),
        check_vma=False,
    )
```

```python
import jax
import jax.numpy as jnp
from jax import lax
from jax.experimental import pallas as pl
from jax.experimental.pallas import tpu as pltpu
from jax.sharding import Mesh, PartitionSpec as P

SIZES = (4, 2, 4, 2, 2)
NAMES = ("x", "zl", "y", "zh", "c")
BF16 = jnp.bfloat16
F32 = jnp.float32


def swapped(value, axis):
    return lax.ppermute(value, axis, [(0, 1), (1, 0)])


def both_swapped(value):
    return lax.ppermute(value, ("zl", "zh"), [(i, 3 - i) for i in range(4)])


def ordered(index, own, other):
    both = jnp.stack([own, other])
    return jnp.where(index == 0, both, both[::-1])


def mm(a, b):
    return lax.dot_general(a, b, (((1,), (0,)), ((), ())), preferred_element_type=F32)


QB = 4


def prepare(w_ref, lows, wt, lower):
    for k in range(8):
        wt[k * 128 : (k + 1) * 128, :] = w_ref[k].T
    for zk in range(2):
        for zd in range(2):
            for j in range(4):
                for e in range(2):
                    row, col = (zk * 4 + j) * 128, (zd * 2 + e) * 128
                    lower[row : row + 128, col : col + 128] = lows[2 * zk + zd][j, e]


def products(zh_ref, uw_ref, acc_ref, out_ref, wt, lower):
    count = uw_ref.shape[0] // 2
    for at in range(0, count, QB):
        u = jnp.concatenate([uw_ref[at + q] for q in range(QB)], axis=1)
        joined = mm(wt[...], u).astype(BF16)
        left = jnp.concatenate(
            [
                jnp.concatenate(
                    [
                        joined[k * 128 : (k + 1) * 128, q * 128 : (q + 1) * 128]
                        for k in range(8)
                    ],
                    axis=1,
                )
                for q in range(QB)
            ],
            axis=0,
        )
        paired = mm(left, lower[...]).astype(BF16)
        rows = jnp.concatenate(
            [
                jnp.concatenate(
                    [
                        paired[q * 128 : (q + 1) * 128, d * 128 : (d + 1) * 128]
                        for q in range(QB)
                    ],
                    axis=1,
                )
                for d in range(4)
            ],
            axis=0,
        )
        slabs = uw_ref[count + at : count + at + QB].reshape(QB * 128, 128)
        part = mm(rows, slabs).reshape(2, 2, 128, 128)
        for zd in range(2):
            to = zh_ref[0] if zd == 0 else 1 - zh_ref[0]
            if at > 0:
                out_ref[to] += part[zd]
            elif acc_ref is None:
                out_ref[to] = part[zd]
            else:
                out_ref[to] = acc_ref[to] + part[zd]


def first_kernel(zh_ref, w_ref, uw_ref, l00, l01, l10, l11, out_ref, wt, lower):
    prepare(w_ref, (l00, l01, l10, l11), wt, lower)
    products(zh_ref, uw_ref, None, out_ref, wt, lower)


def second_kernel(zh_ref, wt, uw_ref, lower, acc_ref, out_ref):
    products(zh_ref, uw_ref, acc_ref, out_ref, wt, lower)


def contract(body, args, outs):
    vmem = pl.BlockSpec(memory_space=pltpu.VMEM)
    return pl.pallas_call(
        body,
        in_specs=[pl.BlockSpec(memory_space=pltpu.SMEM)] + [vmem] * (len(args) - 1),
        out_specs=[vmem] * len(outs),
        out_shape=[jax.ShapeDtypeStruct(*out) for out in outs],
        compiler_params=pltpu.CompilerParams(vmem_limit_bytes=40 * 1024 * 1024),
        cost_estimate=pl.CostEstimate(
            flops=4 * 10**9, bytes_accessed=4 * 2**20, transcendentals=0
        ),
        name="contract",
    )(*args)


def fetch_kernel(*refs):
    count = len(refs) // 3
    copies = [
        pltpu.make_async_copy(refs[i], refs[count + i], refs[2 * count + i])
        for i in range(count)
    ]
    for copy in copies:
        copy.start()
    for copy in copies:
        copy.wait()


def fetched(*arrays):
    return pl.pallas_call(
        fetch_kernel,
        in_specs=[pl.BlockSpec(memory_space=pltpu.HBM)] * len(arrays),
        out_specs=[pl.BlockSpec(memory_space=pltpu.VMEM)] * len(arrays),
        out_shape=[pltpu.VMEM(a.shape, a.dtype) for a in arrays],
        scratch_shapes=[pltpu.SemaphoreType.DMA] * len(arrays),
        name="fetch",
    )(*arrays)


def on_device(upper, lower, isometry):
    isometry, upper, lower = fetched(isometry, upper, lower)
    zl = lax.axis_index("zl")
    zh = lax.axis_index("zh")
    c = lax.axis_index("c")

    lower = lower.transpose(1, 2, 0, 3)
    pair = ordered(c, isometry, swapped(isometry, "c"))

    t = jnp.arange(32)
    plane = jnp.where(t < 16, zl, 1 - zl)
    xy = t % 16
    wanted = 4 * ((xy // 4) * 8 + plane * 4 + xy % 4) + 2 * zh + c
    pick = (wanted[:, None] == jnp.arange(128)[None, :]).astype(BF16)
    rights = jnp.einsum(
        "qr,mlr->qlm", pick, upper, preferred_element_type=F32
    ).astype(BF16)

    theirs = swapped(
        jnp.concatenate([rights[16:].reshape(64, 128), pair.reshape(256, 128)]), "zl"
    )
    far = swapped(pair, "zh"), both_swapped(pair)
    own = ordered(zh, pair, far[0])
    other = ordered(zh, theirs[64:].reshape(2, 128, 128), far[1])
    column = ordered(zl, own, other).reshape(8, 4, 2, 4, 4, 128)
    ks = column.transpose(1, 3, 2, 4, 0, 5)
    ks = jnp.where(zl == 0, ks, ks[:, :, ::-1])

    lowers = (lower, swapped(lower, "zh"), swapped(lower, "zl"), both_swapped(lower))

    theirs = theirs[:64].reshape(16, 4, 128)
    first = jnp.where(zl == 0, rights[:16], theirs)
    second = jnp.where(zl == 0, theirs, rights[:16])
    rights = jnp.concatenate([first, second], axis=1)
    send = jnp.concatenate(
        [
            jnp.broadcast_to(rights.reshape(1, 128, 128), (16, 128, 128)),
            ks.reshape(16, 64, 128),
            jnp.broadcast_to(isometry[None], (16, 128, 128)),
        ],
        axis=1,
    )
    got = lax.all_to_all(send, ("x", "y"), 0, 0, tiled=True)
    mats = got[:, :192].reshape(16, 24, 8, 128).transpose(1, 0, 2, 3).reshape(24, 128, 128)
    uw = jnp.concatenate([mats[:16], got[:, 192:]])
    uw_other = swapped(uw, "c")

    at = zh.astype(jnp.int32)[None]
    total = ((2, 2, 128, 128), F32)
    kept = ((1024, 128), BF16), ((1024, 512), BF16)
    acc, wt, low = contract(
        first_kernel, (at, mats[16:], uw, *lowers), (total, *kept)
    )
    (acc,) = contract(second_kernel, (at, wt, uw_other, low, acc), (total,))

    parts = acc.reshape(2, 2, 32, 4, 128).transpose(2, 0, 1, 3, 4).reshape(64, 8, 128)
    parts = lax.all_to_all(parts, ("x", "zl", "y", "zh"), 0, 0, tiled=True)
    return jnp.sum(parts, axis=0).reshape(2, 4, 128).transpose(1, 0, 2)


def solution(mesh):
    return jax.shard_map(
        on_device,
        mesh=Mesh(mesh.devices.reshape(SIZES), NAMES),
        in_specs=(
            P(None, ("x", "zl", "y"), None),
            P(None, ("x", "zl", "y"), ("zh", "c"), None),
            P(NAMES, None),
        ),
        out_specs=P(("x", "zl", "y"), ("zh", "c"), None),
        check_vma=False,
    )
```

```python
import jax
import jax.numpy as jnp
from jax import lax
from jax.experimental import pallas as pl
from jax.experimental.pallas import tpu as pltpu
from jax.sharding import Mesh, PartitionSpec as P

SIZES = (4, 2, 4, 2, 2)
NAMES = ("x", "zl", "y", "zh", "c")
BF16 = jnp.bfloat16
F32 = jnp.float32


def swapped(value, axis):
    return lax.ppermute(value, axis, [(0, 1), (1, 0)])


def both_swapped(value):
    return lax.ppermute(value, ("zl", "zh"), [(i, 3 - i) for i in range(4)])


def ordered(index, own, other):
    both = jnp.stack([own, other])
    return jnp.where(index == 0, both, both[::-1])


def mm(a, b):
    return lax.dot_general(a, b, (((1,), (0,)), ((), ())), preferred_element_type=F32)


QB = 4


def prepare(w_ref, lows, wt, lower):
    for k in range(8):
        wt[k * 128 : (k + 1) * 128, :] = w_ref[k].T
    for zk in range(2):
        for zd in range(2):
            for j in range(4):
                for e in range(2):
                    row, col = (zk * 4 + j) * 128, (zd * 2 + e) * 128
                    lower[row : row + 128, col : col + 128] = lows[2 * zk + zd][j, e]


def products(zh_ref, uw_ref, acc_ref, out_ref, wt, lower):
    count = uw_ref.shape[0] // 2
    for at in range(0, count, QB):
        u = jnp.concatenate([uw_ref[at + q] for q in range(QB)], axis=1)
        joined = mm(wt[...], u).astype(BF16)
        left = jnp.concatenate(
            [
                jnp.concatenate(
                    [
                        joined[k * 128 : (k + 1) * 128, q * 128 : (q + 1) * 128]
                        for k in range(8)
                    ],
                    axis=1,
                )
                for q in range(QB)
            ],
            axis=0,
        )
        paired = mm(left, lower[...]).astype(BF16)
        rows = jnp.concatenate(
            [
                jnp.concatenate(
                    [
                        paired[q * 128 : (q + 1) * 128, d * 128 : (d + 1) * 128]
                        for q in range(QB)
                    ],
                    axis=1,
                )
                for d in range(4)
            ],
            axis=0,
        )
        slabs = uw_ref[count + at : count + at + QB].reshape(QB * 128, 128)
        part = mm(rows, slabs).reshape(2, 2, 128, 128)
        for zd in range(2):
            to = zh_ref[0] if zd == 0 else 1 - zh_ref[0]
            if at > 0:
                out_ref[to] += part[zd]
            elif acc_ref is None:
                out_ref[to] = part[zd]
            else:
                out_ref[to] = acc_ref[to] + part[zd]


def first_kernel(zh_ref, w_ref, uw_ref, l00, l01, l10, l11, out_ref, wt, lower):
    prepare(w_ref, (l00, l01, l10, l11), wt, lower)
    products(zh_ref, uw_ref, None, out_ref, wt, lower)


def second_kernel(zh_ref, wt, uw_ref, lower, acc_ref, out_ref):
    products(zh_ref, uw_ref, acc_ref, out_ref, wt, lower)


def contract(body, args, outs):
    vmem = pl.BlockSpec(memory_space=pltpu.VMEM)
    return pl.pallas_call(
        body,
        in_specs=[pl.BlockSpec(memory_space=pltpu.SMEM)] + [vmem] * (len(args) - 1),
        out_specs=[vmem] * len(outs),
        out_shape=[jax.ShapeDtypeStruct(*out) for out in outs],
        compiler_params=pltpu.CompilerParams(vmem_limit_bytes=40 * 1024 * 1024),
        cost_estimate=pl.CostEstimate(
            flops=4 * 10**9, bytes_accessed=4 * 2**20, transcendentals=0
        ),
        name="contract",
    )(*args)


def fetch_kernel(*refs):
    count = len(refs) // 3
    copies = [
        pltpu.make_async_copy(refs[i], refs[count + i], refs[2 * count + i])
        for i in range(count)
    ]
    for copy in copies:
        copy.start()
    for copy in copies:
        copy.wait()


def fetched(*arrays):
    return pl.pallas_call(
        fetch_kernel,
        in_specs=[pl.BlockSpec(memory_space=pltpu.HBM)] * len(arrays),
        out_specs=[pl.BlockSpec(memory_space=pltpu.VMEM)] * len(arrays),
        out_shape=[pltpu.VMEM(a.shape, a.dtype) for a in arrays],
        scratch_shapes=[pltpu.SemaphoreType.DMA] * len(arrays),
        name="fetch",
    )(*arrays)


def on_device(upper, lower, isometry):
    isometry, upper, lower = fetched(isometry, upper, lower)
    zl = lax.axis_index("zl")
    zh = lax.axis_index("zh")
    c = lax.axis_index("c")

    lower = lower.transpose(1, 2, 0, 3)
    t = jnp.arange(32)
    plane = jnp.where(t < 16, zl, 1 - zl)
    xy = t % 16
    wanted = 4 * ((xy // 4) * 8 + plane * 4 + xy % 4) + 2 * zh + c
    pick = (wanted[:, None] == jnp.arange(128)[None, :]).astype(BF16)
    rights = jnp.einsum(
        "qr,mlr->qlm", pick, upper, preferred_element_type=F32
    ).astype(BF16)

    theirs = swapped(
        jnp.concatenate([rights[16:].reshape(64, 128), isometry], axis=0), "zl"
    )
    far = swapped(isometry, "zh"), both_swapped(isometry)
    own = ordered(zh, isometry, far[0])
    other = ordered(zh, theirs[64:], far[1])
    column = ordered(zl, own, other).reshape(4, 4, 2, 4, 4, 128)
    ks = column.transpose(1, 3, 2, 4, 0, 5)
    ks = jnp.where(zl == 0, ks, ks[:, :, ::-1])

    l01 = swapped(lower, "zh")
    l10 = swapped(lower, "zl")
    l11 = both_swapped(lower)
    lowers = (lower, l01, l10, l11)

    rights = ordered(zl, rights[:16], theirs[:64].reshape(16, 4, 128))
    rights = rights.reshape(2, 16, 2, 2, 128).transpose(1, 3, 0, 2, 4)
    send = jnp.concatenate(
        [
            jnp.broadcast_to(rights.reshape(1, 128, 128), (16, 128, 128)),
            ks.reshape(16, 32, 128),
            jnp.broadcast_to(isometry[None], (16, 128, 128)),
        ],
        axis=1,
    )
    got = lax.all_to_all(send, ("x", "y"), 0, 0, tiled=True)
    w = got[:, 128:160].reshape(16, 8, 4, 128).transpose(1, 0, 2, 3)
    u = got[:, :128].reshape(16, 16, 8, 128).transpose(1, 0, 2, 3).reshape(16, 128, 128)
    w = ordered(c, w, swapped(w, "c"))
    w = w.transpose(1, 2, 0, 3, 4).reshape(8, 128, 128)
    uw = jnp.concatenate([u, got[:, 160:]])
    uw_other = swapped(uw, "c")

    at = zh.astype(jnp.int32)[None]
    total = ((2, 2, 128, 128), F32)
    kept = ((1024, 128), BF16), ((1024, 512), BF16)
    acc, wt, low = contract(
        first_kernel, (at, w, uw, *lowers), (total, *kept)
    )
    (acc,) = contract(second_kernel, (at, wt, uw_other, low, acc), (total,))

    parts = acc.reshape(2, 2, 32, 4, 128).transpose(2, 0, 1, 3, 4).reshape(64, 8, 128)
    parts = lax.all_to_all(parts, ("x", "zl", "y", "zh"), 0, 0, tiled=True)
    return jnp.sum(parts, axis=0).reshape(2, 4, 128).transpose(1, 0, 2)


def solution(mesh):
    return jax.shard_map(
        on_device,
        mesh=Mesh(mesh.devices.reshape(SIZES), NAMES),
        in_specs=(
            P(None, ("x", "zl", "y"), None),
            P(None, ("x", "zl", "y"), ("zh", "c"), None),
            P(NAMES, None),
        ),
        out_specs=P(("x", "zl", "y"), ("zh", "c"), None),
        check_vma=False,
    )
```

```python
import jax
import jax.numpy as jnp
from jax import lax
from jax.experimental import pallas as pl
from jax.experimental.pallas import tpu as pltpu
from jax.sharding import Mesh, PartitionSpec as P

SIZES = (4, 2, 4, 2, 2)
NAMES = ("x", "zl", "y", "zh", "c")
BF16 = jnp.bfloat16
F32 = jnp.float32


def swapped(value, axis):
    return lax.ppermute(value, axis, [(0, 1), (1, 0)])


def along_z(value, shift):
    def at(z):
        return (z % 2) * 2 + z // 2

    return lax.ppermute(
        value, ("zl", "zh"), [(at(z), at((z + shift) % 4)) for z in range(4)]
    )


def ordered(index, own, other):
    both = jnp.stack([own, other])
    return jnp.where(index == 0, both, both[::-1])


def mm(a, b):
    return lax.dot_general(a, b, (((1,), (0,)), ((), ())), preferred_element_type=F32)


QB = 4


def prepare(z_ref, w_ref, lows, wt, lower):
    for k in range(8):
        wt[k * 128 : (k + 1) * 128, :] = w_ref[k].T
    for shift in range(4):
        z = (z_ref[0] + 4 - shift) % 4
        for j in range(4):
            row = pl.multiple_of(((z % 2) * 4 + j) * 128, 128)
            for e in range(2):
                block = lows[shift][j, e]
                lower[z // 2, pl.ds(row, 128), e * 128 : (e + 1) * 128] = block


def products(uw_ref, acc_ref, out_ref, wt, lower):
    count = uw_ref.shape[0] // 2
    for at in range(0, count, QB):
        u = jnp.concatenate([uw_ref[at + q] for q in range(QB)], axis=1)
        joined = mm(wt[...], u).astype(BF16)
        left = jnp.concatenate(
            [
                jnp.concatenate(
                    [
                        joined[k * 128 : (k + 1) * 128, q * 128 : (q + 1) * 128]
                        for k in range(8)
                    ],
                    axis=1,
                )
                for q in range(QB)
            ],
            axis=0,
        )
        paired = [mm(left, lower[zh]).astype(BF16) for zh in range(2)]
        rows = jnp.concatenate(
            [
                jnp.concatenate(
                    [
                        paired[zh][q * 128 : (q + 1) * 128, e * 128 : (e + 1) * 128]
                        for q in range(QB)
                    ],
                    axis=1,
                )
                for zh in range(2)
                for e in range(2)
            ],
            axis=0,
        )
        slabs = uw_ref[count + at : count + at + QB].reshape(QB * 128, 128)
        part = mm(rows, slabs).reshape(2, 2, 128, 128)
        if at > 0:
            out_ref[...] += part
        elif acc_ref is None:
            out_ref[...] = part
        else:
            out_ref[...] = acc_ref[...] + part


def first_kernel(z_ref, w_ref, uw_ref, l0, l1, l2, l3, out_ref, wt, lower):
    prepare(z_ref, w_ref, (l0, l1, l2, l3), wt, lower)
    products(uw_ref, None, out_ref, wt, lower)


def second_kernel(z_ref, wt, uw_ref, lower, acc_ref, out_ref):
    products(uw_ref, acc_ref, out_ref, wt, lower)


def contract(body, args, outs):
    vmem = pl.BlockSpec(memory_space=pltpu.VMEM)
    return pl.pallas_call(
        body,
        in_specs=[pl.BlockSpec(memory_space=pltpu.SMEM)] + [vmem] * (len(args) - 1),
        out_specs=[vmem] * len(outs),
        out_shape=[jax.ShapeDtypeStruct(*out) for out in outs],
        compiler_params=pltpu.CompilerParams(vmem_limit_bytes=40 * 1024 * 1024),
        cost_estimate=pl.CostEstimate(
            flops=4 * 10**9, bytes_accessed=4 * 2**20, transcendentals=0
        ),
        name="contract",
    )(*args)


def fetch_kernel(*refs):
    count = len(refs) // 3
    copies = [
        pltpu.make_async_copy(refs[i], refs[count + i], refs[2 * count + i])
        for i in range(count)
    ]
    for copy in copies:
        copy.start()
    for copy in copies:
        copy.wait()


def fetched(*arrays):
    return pl.pallas_call(
        fetch_kernel,
        in_specs=[pl.BlockSpec(memory_space=pltpu.HBM)] * len(arrays),
        out_specs=[pl.BlockSpec(memory_space=pltpu.VMEM)] * len(arrays),
        out_shape=[pltpu.VMEM(a.shape, a.dtype) for a in arrays],
        scratch_shapes=[pltpu.SemaphoreType.DMA] * len(arrays),
        name="fetch",
    )(*arrays)


def on_device(upper, lower, isometry):
    isometry, upper, lower = fetched(isometry, upper, lower)
    zl = lax.axis_index("zl")
    zh = lax.axis_index("zh")
    c = lax.axis_index("c")

    lower = lower.transpose(1, 2, 0, 3)
    t = jnp.arange(32)
    plane = jnp.where(t < 16, zl, 1 - zl)
    xy = t % 16
    wanted = 4 * ((xy // 4) * 8 + plane * 4 + xy % 4) + 2 * zh + c
    pick = (wanted[:, None] == jnp.arange(128)[None, :]).astype(BF16)
    rights = jnp.einsum(
        "qr,mlr->qlm", pick, upper, preferred_element_type=F32
    ).astype(BF16)

    both = jnp.concatenate([rights[16:].reshape(64, 128), isometry], axis=0)
    before, after, across = along_z(both, 1), along_z(both, 3), along_z(isometry, 2)
    column = jnp.stack([isometry, after[64:], across, before[64:]])
    column = jnp.where(zl == 0, column, jnp.roll(column, 1, axis=0))
    column = jnp.where(zh == 0, column, jnp.roll(column, 2, axis=0))
    column = lax.optimization_barrier(column).reshape(4, 4, 2, 4, 4, 128)
    ks = column.transpose(1, 3, 2, 4, 0, 5)

    lowers = (lower, along_z(lower, 1), along_z(lower, 2), along_z(lower, 3))

    theirs = jnp.where(zl == 0, after[:64], before[:64]).reshape(16, 4, 128)
    rights = ordered(zl, rights[:16], theirs)
    rights = rights.reshape(2, 16, 2, 2, 128).transpose(1, 3, 2, 0, 4)
    send = jnp.concatenate(
        [
            jnp.broadcast_to(rights.reshape(1, 128, 128), (16, 128, 128)),
            ks.reshape(16, 32, 128),
            jnp.broadcast_to(isometry[None], (16, 128, 128)),
        ],
        axis=1,
    )
    got = lax.all_to_all(send, ("x", "y"), 0, 0, tiled=True)
    w = got[:, 128:160].reshape(16, 8, 4, 128).transpose(1, 0, 2, 3)
    u = got[:, :128].reshape(16, 16, 8, 128).transpose(1, 0, 2, 3).reshape(16, 128, 128)
    w = ordered(c, w, swapped(w, "c"))
    w = w.transpose(1, 2, 0, 3, 4).reshape(8, 128, 128)
    uw = jnp.concatenate([u, got[:, 160:]])
    uw_other = swapped(uw, "c")

    at = (2 * zh + zl).astype(jnp.int32)[None]
    total = ((2, 2, 128, 128), F32)
    kept = ((1024, 128), BF16), ((2, 1024, 256), BF16)
    acc, wt, low = contract(
        first_kernel, (at, w, uw, *lowers), (total, *kept)
    )
    (acc,) = contract(second_kernel, (at, wt, uw_other, low, acc), (total,))

    parts = acc.reshape(2, 2, 32, 4, 128).transpose(2, 0, 1, 3, 4).reshape(64, 8, 128)
    parts = lax.all_to_all(parts, ("x", "zl", "y", "zh"), 0, 0, tiled=True)
    return jnp.sum(parts, axis=0).reshape(2, 4, 128).transpose(1, 0, 2)


def solution(mesh):
    return jax.shard_map(
        on_device,
        mesh=Mesh(mesh.devices.reshape(SIZES), NAMES),
        in_specs=(
            P(None, ("x", "zl", "y"), None),
            P(None, ("x", "zl", "y"), ("zh", "c"), None),
            P(NAMES, None),
        ),
        out_specs=P(("x", "zl", "y"), ("zh", "c"), None),
        check_vma=False,
    )
```

```python
import jax
import jax.numpy as jnp
from jax import lax
from jax.experimental import pallas as pl
from jax.experimental.pallas import tpu as pltpu
from jax.sharding import Mesh, PartitionSpec as P

SIZES = (4, 2, 4, 2, 2)
NAMES = ("x", "zl", "y", "zh", "c")
BF16 = jnp.bfloat16
F32 = jnp.float32


def swapped(value, axis):
    return lax.ppermute(value, axis, [(0, 1), (1, 0)])


def along_z(value, shift):
    def at(z):
        return (z % 2) * 2 + z // 2

    return lax.ppermute(
        value, ("zl", "zh"), [(at(z), at((z + shift) % 4)) for z in range(4)]
    )


def ordered(index, own, other):
    both = jnp.stack([own, other])
    return jnp.where(index == 0, both, both[::-1])


def mm(a, b):
    return lax.dot_general(a, b, (((1,), (0,)), ((), ())), preferred_element_type=F32)


QB = 4


def prepare(z_ref, w_ref, lows, wt, lower):
    for k in range(8):
        wt[k * 128 : (k + 1) * 128, :] = w_ref[k].T

    def place(ref, row, col):
        for j in range(4):
            for e in range(2):
                rows = slice(row + j * 128, row + (j + 1) * 128)
                lower[rows, col + e * 128 : col + (e + 1) * 128] = ref[j, e]

    here, before, across, after = lows
    place(here, 0, 0)
    place(across, 0, 256)

    @pl.when(z_ref[0] == 0)
    def _():
        place(after, 512, 0)
        place(before, 512, 256)

    @pl.when(z_ref[0] != 0)
    def _():
        place(before, 512, 0)
        place(after, 512, 256)


def products(zh, uw_ref, acc_ref, out_ref, wt, lower):
    count = uw_ref.shape[0] // 2
    for at in range(0, count, QB):
        u = jnp.concatenate([uw_ref[at + q] for q in range(QB)], axis=1)
        joined = mm(wt[...], u).astype(BF16)
        left = jnp.concatenate(
            [
                jnp.concatenate(
                    [
                        joined[k * 128 : (k + 1) * 128, q * 128 : (q + 1) * 128]
                        for k in range(8)
                    ],
                    axis=1,
                )
                for q in range(QB)
            ],
            axis=0,
        )
        paired = mm(left, lower[...]).astype(BF16)
        rows = jnp.concatenate(
            [
                jnp.concatenate(
                    [
                        paired[q * 128 : (q + 1) * 128, d * 128 : (d + 1) * 128]
                        for q in range(QB)
                    ],
                    axis=1,
                )
                for d in range(4)
            ],
            axis=0,
        )
        slabs = uw_ref[count + at : count + at + QB].reshape(QB * 128, 128)
        part = mm(rows, slabs).reshape(2, 2, 128, 128)
        for zd in range(2):
            to = zh if zd == 0 else 1 - zh
            if at > 0:
                out_ref[to] += part[zd]
            elif acc_ref is None:
                out_ref[to] = part[zd]
            else:
                out_ref[to] = acc_ref[to] + part[zd]


def first_kernel(z_ref, w_ref, uw_ref, l0, l1, l2, l3, out_ref, wt, lower):
    prepare(z_ref, w_ref, (l0, l1, l2, l3), wt, lower)
    products(z_ref[1], uw_ref, None, out_ref, wt, lower)


def second_kernel(z_ref, wt, uw_ref, lower, acc_ref, out_ref):
    products(z_ref[1], uw_ref, acc_ref, out_ref, wt, lower)


def contract(body, args, outs):
    vmem = pl.BlockSpec(memory_space=pltpu.VMEM)
    return pl.pallas_call(
        body,
        in_specs=[pl.BlockSpec(memory_space=pltpu.SMEM)] + [vmem] * (len(args) - 1),
        out_specs=[vmem] * len(outs),
        out_shape=[jax.ShapeDtypeStruct(*out) for out in outs],
        compiler_params=pltpu.CompilerParams(vmem_limit_bytes=40 * 1024 * 1024),
        cost_estimate=pl.CostEstimate(
            flops=4 * 10**9, bytes_accessed=4 * 2**20, transcendentals=0
        ),
        name="contract",
    )(*args)


def fetch_kernel(*refs):
    count = len(refs) // 3
    copies = [
        pltpu.make_async_copy(refs[i], refs[count + i], refs[2 * count + i])
        for i in range(count)
    ]
    for copy in copies:
        copy.start()
    for copy in copies:
        copy.wait()


def fetched(*arrays):
    return pl.pallas_call(
        fetch_kernel,
        in_specs=[pl.BlockSpec(memory_space=pltpu.HBM)] * len(arrays),
        out_specs=[pl.BlockSpec(memory_space=pltpu.VMEM)] * len(arrays),
        out_shape=[pltpu.VMEM(a.shape, a.dtype) for a in arrays],
        scratch_shapes=[pltpu.SemaphoreType.DMA] * len(arrays),
        name="fetch",
    )(*arrays)


def on_device(upper, lower, isometry):
    isometry, upper, lower = fetched(isometry, upper, lower)
    zl = lax.axis_index("zl")
    zh = lax.axis_index("zh")
    c = lax.axis_index("c")

    lower = lower.transpose(1, 2, 0, 3)
    t = jnp.arange(32)
    plane = jnp.where(t < 16, zl, 1 - zl)
    xy = t % 16
    wanted = 4 * ((xy // 4) * 8 + plane * 4 + xy % 4) + 2 * zh + c
    pick = (wanted[:, None] == jnp.arange(128)[None, :]).astype(BF16)
    rights = jnp.einsum(
        "qr,mlr->qlm", pick, upper, preferred_element_type=F32
    ).astype(BF16)

    both = jnp.concatenate([rights[16:].reshape(64, 128), isometry], axis=0)
    before, after, across = along_z(both, 1), along_z(both, 3), along_z(isometry, 2)
    column = jnp.stack([isometry, after[64:], across, before[64:]])
    column = jnp.where(zl == 0, column, jnp.roll(column, 1, axis=0))
    column = jnp.where(zh == 0, column, jnp.roll(column, 2, axis=0))
    column = lax.optimization_barrier(column).reshape(4, 4, 2, 4, 4, 128)
    ks = column.transpose(1, 3, 2, 4, 0, 5)
    ks = jnp.where(zl == 0, ks, ks[:, :, ::-1])

    lowers = (lower, along_z(lower, 1), along_z(lower, 2), along_z(lower, 3))

    theirs = jnp.where(zl == 0, after[:64], before[:64]).reshape(16, 4, 128)
    rights = ordered(zl, rights[:16], theirs)
    rights = rights.reshape(2, 16, 2, 2, 128).transpose(1, 3, 2, 0, 4)
    send = jnp.concatenate(
        [
            jnp.broadcast_to(rights.reshape(1, 128, 128), (16, 128, 128)),
            ks.reshape(16, 32, 128),
            jnp.broadcast_to(isometry[None], (16, 128, 128)),
        ],
        axis=1,
    )
    got = lax.all_to_all(send, ("x", "y"), 0, 0, tiled=True)
    w = got[:, 128:160].reshape(16, 8, 4, 128).transpose(1, 0, 2, 3)
    u = got[:, :128].reshape(16, 16, 8, 128).transpose(1, 0, 2, 3).reshape(16, 128, 128)
    other = swapped(w, "c")
    w = jnp.concatenate(
        [jnp.where(c == 0, w, other), jnp.where(c == 0, other, w)], axis=2
    ).reshape(8, 128, 128)
    uw = jnp.concatenate([u, got[:, 160:]])
    uw_other = swapped(uw, "c")

    at = jnp.stack([zl, zh]).astype(jnp.int32)
    total = ((2, 2, 128, 128), F32)
    kept = ((1024, 128), BF16), ((1024, 512), BF16)
    acc, wt, low = contract(
        first_kernel, (at, w, uw, *lowers), (total, *kept)
    )
    (acc,) = contract(second_kernel, (at, wt, uw_other, low, acc), (total,))

    parts = acc.reshape(2, 2, 32, 4, 128).transpose(2, 0, 1, 3, 4).reshape(64, 8, 128)
    parts = lax.all_to_all(parts, ("x", "zl", "y", "zh"), 0, 0, tiled=True)
    return jnp.sum(parts, axis=0).reshape(2, 4, 128).transpose(1, 0, 2)


def solution(mesh):
    return jax.shard_map(
        on_device,
        mesh=Mesh(mesh.devices.reshape(SIZES), NAMES),
        in_specs=(
            P(None, ("x", "zl", "y"), None),
            P(None, ("x", "zl", "y"), ("zh", "c"), None),
            P(NAMES, None),
        ),
        out_specs=P(("x", "zl", "y"), ("zh", "c"), None),
        check_vma=False,
    )
```

```python
import jax
import jax.numpy as jnp
from jax import lax
from jax.experimental import pallas as pl
from jax.experimental.pallas import tpu as pltpu
from jax.sharding import Mesh, PartitionSpec as P

SIZES = (4, 2, 4, 2, 2)
NAMES = ("x", "zl", "y", "zh", "c")
BF16 = jnp.bfloat16
F32 = jnp.float32


def swapped(value, axis):
    return lax.ppermute(value, axis, [(0, 1), (1, 0)])


def along_z(value, shift):
    def at(z):
        return (z % 2) * 2 + z // 2

    return lax.ppermute(
        value, ("zl", "zh"), [(at(z), at((z + shift) % 4)) for z in range(4)]
    )


def ordered(index, own, other):
    both = jnp.stack([own, other])
    return jnp.where(index == 0, both, both[::-1])


def mm(a, b):
    return lax.dot_general(a, b, (((1,), (0,)), ((), ())), preferred_element_type=F32)


QB = 4


def prepare(zl, w_ref, lows, wt, lower):
    for k in range(8):
        wt[k * 128 : (k + 1) * 128, :] = w_ref[k].T

    def place(ref, row, col):
        for j in range(4):
            for e in range(2):
                rows = slice(row + j * 128, row + (j + 1) * 128)
                lower[rows, col + e * 128 : col + (e + 1) * 128] = ref[j, e]

    here, before, across, after = lows
    place(here, 0, 0)
    place(across, 0, 256)

    @pl.when(zl == 0)
    def _():
        place(after, 512, 0)
        place(before, 512, 256)

    @pl.when(zl != 0)
    def _():
        place(before, 512, 0)
        place(after, 512, 256)


def products(zh, uw_ref, acc_ref, out_ref, wt, lower):
    count = uw_ref.shape[0] // 2
    for at in range(0, count, QB):
        u = jnp.concatenate([uw_ref[at + q] for q in range(QB)], axis=1)
        joined = mm(wt[...], u).astype(BF16)
        left = jnp.concatenate(
            [
                jnp.concatenate(
                    [
                        joined[k * 128 : (k + 1) * 128, q * 128 : (q + 1) * 128]
                        for k in range(8)
                    ],
                    axis=1,
                )
                for q in range(QB)
            ],
            axis=0,
        )
        paired = mm(left, lower[...]).astype(BF16)
        rows = jnp.concatenate(
            [
                jnp.concatenate(
                    [
                        paired[q * 128 : (q + 1) * 128, d * 128 : (d + 1) * 128]
                        for q in range(QB)
                    ],
                    axis=1,
                )
                for d in range(4)
            ],
            axis=0,
        )
        slabs = uw_ref[count + at : count + at + QB].reshape(QB * 128, 128)
        part = mm(rows, slabs).reshape(2, 2, 128, 128)
        for zd in range(2):
            to = zh if zd == 0 else 1 - zh
            if at > 0:
                out_ref[to] += part[zd]
            elif acc_ref is None:
                out_ref[to] = part[zd]
            else:
                out_ref[to] = acc_ref[to] + part[zd]


def first_kernel(zl_ref, zh_ref, w_ref, uw_ref, l0, l1, l2, l3, out_ref, wt, lower):
    prepare(zl_ref[0], w_ref, (l0, l1, l2, l3), wt, lower)
    products(zh_ref[0], uw_ref, None, out_ref, wt, lower)


def second_kernel(zh_ref, wt, uw_ref, lower, acc_ref, out_ref):
    products(zh_ref[0], uw_ref, acc_ref, out_ref, wt, lower)


def contract(body, scalars, args, outs):
    vmem = pl.BlockSpec(memory_space=pltpu.VMEM)
    return pl.pallas_call(
        body,
        in_specs=[pl.BlockSpec(memory_space=pltpu.SMEM)] * len(scalars) + [vmem] * len(args),
        out_specs=[vmem] * len(outs),
        out_shape=[jax.ShapeDtypeStruct(*out) for out in outs],
        compiler_params=pltpu.CompilerParams(vmem_limit_bytes=40 * 1024 * 1024),
        cost_estimate=pl.CostEstimate(
            flops=4 * 10**9, bytes_accessed=4 * 2**20, transcendentals=0
        ),
        name="contract",
    )(*scalars, *args)


def fetch_kernel(*refs):
    count = len(refs) // 3
    copies = [
        pltpu.make_async_copy(refs[i], refs[count + i], refs[2 * count + i])
        for i in range(count)
    ]
    for copy in copies:
        copy.start()
    for copy in copies:
        copy.wait()


def fetched(*arrays):
    return pl.pallas_call(
        fetch_kernel,
        in_specs=[pl.BlockSpec(memory_space=pltpu.HBM)] * len(arrays),
        out_specs=[pl.BlockSpec(memory_space=pltpu.VMEM)] * len(arrays),
        out_shape=[pltpu.VMEM(a.shape, a.dtype) for a in arrays],
        scratch_shapes=[pltpu.SemaphoreType.DMA] * len(arrays),
        name="fetch",
    )(*arrays)


def on_device(upper, lower, isometry):
    isometry, upper, lower = fetched(isometry, upper, lower)
    zl = lax.axis_index("zl")
    zh = lax.axis_index("zh")
    c = lax.axis_index("c")

    lower = lower.transpose(1, 2, 0, 3)
    t = jnp.arange(32)
    plane = jnp.where(t < 16, zl, 1 - zl)
    xy = t % 16
    wanted = 4 * ((xy // 4) * 8 + plane * 4 + xy % 4) + 2 * zh + c
    pick = (wanted[:, None] == jnp.arange(128)[None, :]).astype(BF16)
    rights = jnp.einsum(
        "qr,mlr->qlm", pick, upper, preferred_element_type=F32
    ).astype(BF16)

    both = jnp.concatenate([rights[16:].reshape(64, 128), isometry], axis=0)
    before, after, across = along_z(both, 1), along_z(both, 3), along_z(isometry, 2)
    column = jnp.stack([isometry, after[64:], across, before[64:]])
    column = jnp.where(zl == 0, column, jnp.roll(column, 1, axis=0))
    column = jnp.where(zh == 0, column, jnp.roll(column, 2, axis=0))
    column = lax.optimization_barrier(column).reshape(4, 4, 2, 4, 4, 128)
    ks = column.transpose(1, 3, 2, 4, 0, 5)
    ks = jnp.where(zl == 0, ks, ks[:, :, ::-1])

    lowers = (lower, along_z(lower, 1), along_z(lower, 2), along_z(lower, 3))

    theirs = jnp.where(zl == 0, after[:64], before[:64]).reshape(16, 4, 128)
    rights = ordered(zl, rights[:16], theirs)
    rights = rights.reshape(2, 16, 2, 2, 128).transpose(1, 3, 2, 0, 4)
    send = jnp.concatenate(
        [
            jnp.broadcast_to(rights.reshape(1, 128, 128), (16, 128, 128)),
            ks.reshape(16, 32, 128),
            jnp.broadcast_to(isometry[None], (16, 128, 128)),
        ],
        axis=1,
    )
    got = lax.all_to_all(send, ("x", "y"), 0, 0, tiled=True)
    w = got[:, 128:160].reshape(16, 8, 4, 128).transpose(1, 0, 2, 3)
    u = got[:, :128].reshape(16, 16, 8, 128).transpose(1, 0, 2, 3).reshape(16, 128, 128)
    other = swapped(w, "c")
    w = jnp.concatenate(
        [jnp.where(c == 0, w, other), jnp.where(c == 0, other, w)], axis=2
    ).reshape(8, 128, 128)
    uw = jnp.concatenate([u, got[:, 160:]])
    uw_other = swapped(uw, "c")

    here, there = zl.astype(jnp.int32)[None], zh.astype(jnp.int32)[None]
    total = ((2, 2, 128, 128), F32)
    kept = ((1024, 128), BF16), ((1024, 512), BF16)
    acc, wt, low = contract(
        first_kernel, (here, there), (w, uw, *lowers), (total, *kept)
    )
    (acc,) = contract(second_kernel, (there,), (wt, uw_other, low, acc), (total,))

    parts = acc.reshape(2, 2, 32, 4, 128).transpose(2, 0, 1, 3, 4).reshape(64, 8, 128)
    parts = lax.all_to_all(parts, ("x", "zl", "y", "zh"), 0, 0, tiled=True)
    return jnp.sum(parts, axis=0).reshape(2, 4, 128).transpose(1, 0, 2)


def solution(mesh):
    return jax.shard_map(
        on_device,
        mesh=Mesh(mesh.devices.reshape(SIZES), NAMES),
        in_specs=(
            P(None, ("x", "zl", "y"), None),
            P(None, ("x", "zl", "y"), ("zh", "c"), None),
            P(NAMES, None),
        ),
        out_specs=P(("x", "zl", "y"), ("zh", "c"), None),
        check_vma=False,
    )
```
